32 devices in a mesh: phi: 4 (over z), row: 2 (over core), theta: 4 (over y, x).
Axes of the slice: x: 2, y: 2, z: 4, core: 2. Of those that a mesh axis runs over, the one named last changes fastest.
Arguments:
- density: float32 [16, 32, 512], P('theta', 'row', 'phi'), may hold values from 0.5 to 2
- energy: float32 [16, 32, 512], P('theta', 'row', 'phi'), may hold values from 0.5 to 2.5
- velocity: float32 [3, 16, 32, 512], P(None, 'theta', 'row', 'phi'), may hold values from -1.2 to 1.2
- shifts: int32 [32], P('row'), may hold values from 0 to 511, as said below
- viscosity: float32 [32], P('row'), may hold values from 0.05 to 0.3
Outputs:
- density_out: float32 [16, 32, 512], P('theta', 'row', 'phi')
- energy_out: float32 [16, 32, 512], P('theta', 'row', 'phi')
- velocity_out: float32 [3, 16, 32, 512], P(None, 'theta', 'row', 'phi')
The draws below stay inside these ranges and needn't reach their ends.
Inputs may be any that keep to these rules, and one draw needn't show every extreme that they name: `shifts`: in each aligned block of 16 radii at least one radius has an offset between 192 and 319, and at least one radius has an offset between 1 and 64.
All inputs are finite; a program needn't handle non-finite values.
Results may differ from the reference program's by a relative error of at most 0.00002.
Values sent between devices are 32-bit elements; how exact they have to be, the bound alone decides.
A program may use at most 64 MiB of HBM per device.

```python
import math
import jax
import jax.numpy as jnp
from jax import lax

CPHI = 128
CR = 16
NPHI = 512
NR = 32
NTH = 16


def draw_shifts(key, part):
    base_key = jax.random.fold_in(key, 7)
    key_base, key_near, key_pick, key_small, key_other = jax.random.split(base_key, 5)
    uniform_shift = jax.random.randint(key_base, (NR,), 0, NPHI)
    near_half = NPHI // 2 + jax.random.randint(key_near, (NR,), -(CPHI // 2), CPHI // 2)
    small_shift = 1 + jax.random.randint(key_small, (NR,), 0, CPHI // 2)
    picked = jax.random.randint(key_pick, (NR // CR,), 0, CR)
    other = (picked + 1 + jax.random.randint(key_other, (NR // CR,), 0, CR - 1)) % CR
    within = lax.iota(jnp.int32, NR) % CR
    chosen = within == jnp.repeat(picked, CR, total_repeat_length=NR)
    second = within == jnp.repeat(other, CR, total_repeat_length=NR)
    result = jnp.where(chosen, near_half, jnp.where(second, small_shift, uniform_shift))
    return result.astype(jnp.int32)


def steps_of(key, shape, cuts, smallest, top_value):
    gain = 1.0
    for position, shards_of in cuts:
        steps = jax.random.uniform(jax.random.fold_in(jax.random.fold_in(key, 6), position), (shards_of,), jnp.float32, smallest / len(cuts), top_value / len(cuts))
        gain = gain * jnp.repeat(jnp.exp(steps), shape[position] // shards_of).reshape((-1,) + (1,) * (len(shape) - 1 - position))
    return gain


def gaussian(rng, extent, scale, reach, cuts=(), dtype=jnp.bfloat16):
    values = scale * jax.random.normal(rng, extent, jnp.float32)
    if cuts:
        values = values * steps_of(rng, extent, cuts, -0.22, 0.18)
    return jnp.clip(values, -reach, reach).astype(dtype)


def setup_inputs(seed: int = 0) -> dict:
    splits = jax.random.split(jax.random.key(seed), 6)
    density = jnp.clip(jnp.exp(math.log(2.0) - 1.3862944 * jax.random.uniform(splits[0], (NTH, NR, NPHI), jnp.float32) ** steps_of(splits[0], (NTH, NR, NPHI), ((0, 4), (1, 2), (2, 4)), -0.2, 0.2)), 0.5, 2.0)
    energy = jnp.clip(jnp.exp(math.log(2.5) - 1.609438 * jax.random.uniform(splits[1], (NTH, NR, NPHI), jnp.float32) ** steps_of(splits[1], (NTH, NR, NPHI), ((0, 4), (1, 2), (2, 4)), -0.2, 0.2)), 0.5, 2.5)
    velocity = gaussian(splits[2], (3, NTH, NR, NPHI), 0.3, 1.2, ((1, 4), (2, 2), (3, 4)), jnp.float32)
    shifts = draw_shifts(jax.random.fold_in(splits[5], 71), 0)
    viscosity = jnp.clip(jnp.exp(math.log(0.3) - 1.7917595 * jax.random.uniform(splits[4], (NR,), jnp.float32) ** steps_of(splits[4], (NR,), ((0, 2),), -0.2, 0.2)), 0.05, 0.3)
    return dict(density=density, energy=energy, velocity=velocity, shifts=shifts, viscosity=viscosity)


GAMMA_LESS = 0.4
TIME_STEP = 0.4
DAMPING = 1.0
ROTATION = 0.5


def face_flux(quantity_lo, quantity_hi, speed_lo, speed_hi):
    return 0.25 * (speed_lo + speed_hi) * (quantity_lo + quantity_hi) - 0.5 * DAMPING * (quantity_hi - quantity_lo)


def segment_rates(padded, inv_rho):
    density, energy, radial_v, polar_v, azimuth_v = padded[0], padded[1], padded[2], padded[3], padded[4]

    def interior(quantity):
        return quantity[1:-1, 1:-1]

    def radial(quantity):
        fluxes = face_flux(quantity[1:-1, :-1], quantity[1:-1, 1:], radial_v[1:-1, :-1], radial_v[1:-1, 1:])
        return fluxes[:, 1:] - fluxes[:, :-1]

    def polar(quantity):
        fluxes = face_flux(quantity[:-1, 1:-1], quantity[1:, 1:-1], polar_v[:-1, 1:-1], polar_v[1:, 1:-1])
        return fluxes[1:] - fluxes[:-1]

    def laplace(quantity):
        return quantity[2:, 1:-1] + quantity[:-2, 1:-1] + quantity[1:-1, 2:] + quantity[1:-1, :-2] - 4.0 * interior(quantity)

    pressure = GAMMA_LESS * energy
    grad_radial = 0.5 * (pressure[1:-1, 2:] - pressure[1:-1, :-2])
    grad_polar = 0.5 * (pressure[2:, 1:-1] - pressure[:-2, 1:-1])
    rate_rho = -(radial(density) + polar(density))
    rate_energy = -(radial(energy) + polar(energy))
    rate_radial = -grad_radial * inv_rho + 0.5 * DAMPING * laplace(radial_v) + 2.0 * ROTATION * interior(azimuth_v)
    rate_polar = -grad_polar * inv_rho + 0.5 * DAMPING * laplace(polar_v)
    rate_azimuth = -(radial(azimuth_v) + polar(azimuth_v)) - 0.5 * ROTATION * interior(radial_v)
    return jnp.stack([rate_rho, rate_energy, rate_radial, rate_polar, rate_azimuth])


def reference(density, energy, velocity, shifts, viscosity):
    fields = jnp.concatenate([density[None], energy[None], velocity], 0)
    inv_rho = 1.0 / density

    def apply_rates(current):
        padded = jnp.pad(current, ((0, 0), (1, 1), (1, 1), (0, 0)))
        return segment_rates(padded, inv_rho)

    segment_one = fields + TIME_STEP * apply_rates(fields)
    segment_two = 0.5 * (fields + segment_one + TIME_STEP * apply_rates(segment_one))
    shifted = jax.vmap(lambda annulus, offset: jnp.roll(annulus, offset, axis=-1), in_axes=(2, 0), out_axes=2)(segment_two, shifts)
    behind = jnp.roll(shifted, 1, axis=-1)
    ahead = jnp.roll(shifted, -1, axis=-1)
    visc_coef = viscosity[None, :, None]
    velocity_out = shifted[2:] + visc_coef * (ahead[2:] - 2.0 * shifted[2:] + behind[2:])
    azimuth_slope = 0.5 * (ahead[4] - behind[4])
    energy_out = shifted[1] + visc_coef * shifted[0] * azimuth_slope * azimuth_slope
    return shifted[0], energy_out, velocity_out
```

```python
import functools

import jax
import jax.numpy as jnp
from jax import lax
from jax.experimental import pallas as pl
from jax.experimental.pallas import tpu as pltpu
from jax.sharding import PartitionSpec as P

GAMMA_LESS = 0.4
TIME_STEP = 0.4
DAMPING = 1.0
ROTATION = 0.5
TILE = 8
FIELDS = 5
MESH = pl.DeviceIdType.MESH


def face_flux(quantity_lo, quantity_hi, speed_lo, speed_hi):
    return 0.25 * (speed_lo + speed_hi) * (quantity_lo + quantity_hi) - 0.5 * DAMPING * (
        quantity_hi - quantity_lo
    )


def rates(src, t, first, count, inv_rho):
    def layer(step_t, step_r):
        return [src[f, t + step_t, pl.ds(first + step_r, count)] for f in range(FIELDS)]

    mid, inner, outer = layer(0, 0), layer(0, -1), layer(0, 1)
    low, high = layer(-1, 0), layer(1, 0)

    def div(q):
        return (
            face_flux(mid[q], outer[q], mid[2], outer[2])
            - face_flux(inner[q], mid[q], inner[2], mid[2])
        ) + (face_flux(mid[q], high[q], mid[3], high[3]) - face_flux(low[q], mid[q], low[3], mid[3]))

    def laplace(q):
        return high[q] + low[q] + outer[q] + inner[q] - 4.0 * mid[q]

    grad_radial = 0.5 * (GAMMA_LESS * outer[1] - GAMMA_LESS * inner[1])
    grad_polar = 0.5 * (GAMMA_LESS * high[1] - GAMMA_LESS * low[1])
    out = [
        -div(0),
        -div(1),
        -grad_radial * inv_rho + 0.5 * DAMPING * laplace(2) + 2.0 * ROTATION * mid[4],
        -grad_polar * inv_rho + 0.5 * DAMPING * laplace(3),
        -div(4) - 0.5 * ROTATION * mid[2],
    ]
    return mid, out


def kernel(
    sizes,
    shifts,
    viscosity,
    density,
    energy,
    velocity,
    density_out,
    energy_out,
    velocity_out,
    state,
    mid_state,
    ring,
    halo_send,
    halo_recv,
    ring_send,
    ring_recv,
):
    n_phi, n_row, n_theta = sizes
    slabs, rows, lanes = density.shape
    phi, row, theta = (lax.axis_index(a) for a in ("phi", "row", "theta"))
    own_t, own_r = pl.ds(2, slabs), pl.ds(TILE, rows)
    ahead_phi = lax.rem(phi + 1, n_phi)
    back_phi = lax.rem(phi + n_phi - 1, n_phi)

    steps = [(0, 1), (0, -1), (1, 1), (1, -1), (-1, 1), (-1, -1), (1, 0), (-1, 0)]
    if n_row == 1:
        steps = [s for s in steps if s[0] == 0]
    if n_theta == 1:
        steps = [s for s in steps if s[1] == 0]

    def exists(step):
        r, t = row + step[0], theta + step[1]
        return (r >= 0) & (r < n_row) & (t >= 0) & (t < n_theta)

    barrier = pltpu.get_barrier_semaphore()
    for step in steps:

        @pl.when(exists(step))
        def _():
            pl.semaphore_signal(
                barrier,
                inc=1,
                device_id={"row": row + step[0], "theta": theta + step[1]},
                device_id_type=MESH,
            )

    if n_phi > 1:
        for other in (ahead_phi, back_phi):
            pl.semaphore_signal(barrier, inc=1, device_id={"phi": other}, device_id_type=MESH)

    state[0, own_t, own_r] = density[...]
    state[1, own_t, own_r] = energy[...]
    for f in range(3):
        state[2 + f, own_t, own_r] = velocity[f]

    def region(step):
        r, t = step
        src_r = {0: pl.ds(0, rows), 1: pl.ds(rows - TILE, TILE), -1: pl.ds(0, TILE)}[r]
        dst_r = {0: own_r, 1: pl.ds(0, TILE), -1: pl.ds(TILE + rows, TILE)}[r]
        deep = 2 if r == 0 else 1
        src_t = {0: pl.ds(0, slabs), 1: pl.ds(slabs - deep, deep), -1: pl.ds(0, deep)}[t]
        dst_t = {0: own_t, 1: pl.ds(2 - deep, deep), -1: pl.ds(2 + slabs, deep)}[t]
        return src_t, src_r, dst_t, dst_r

    def copies(step):
        k = steps.index(step)
        src_t, src_r, dst_t, dst_r = region(step)
        pairs = [
            (density.at[src_t, src_r], state.at[0, dst_t, dst_r]),
            (energy.at[src_t, src_r], state.at[1, dst_t, dst_r]),
            (velocity.at[:, src_t, src_r], state.at[pl.ds(2, 3), dst_t, dst_r]),
        ]
        return [
            pltpu.make_async_remote_copy(
                src_ref=src,
                dst_ref=dst,
                send_sem=halo_send.at[k, i],
                recv_sem=halo_recv.at[k, i],
                device_id={"row": row + step[0], "theta": theta + step[1]},
                device_id_type=MESH,
            )
            for i, (src, dst) in enumerate(pairs)
        ]

    zero_from = [(0, 1), (0, -1), (1, 1), (1, -1), (-1, 1), (-1, -1), (1, 0), (-1, 0)]
    for step in zero_from:
        _, _, dst_t, dst_r = region(step)
        opposite = (-step[0], -step[1])

        def clear():
            for f in range(FIELDS):
                state[f, dst_t, dst_r] = jnp.zeros((dst_t.size, dst_r.size, lanes), jnp.float32)

        if opposite in steps:
            pl.when(jnp.logical_not(exists(opposite)))(clear)
        else:
            clear()

    expected = 2 if n_phi > 1 else 0
    for step in steps:
        expected = expected + exists(step).astype(jnp.int32)
    pl.semaphore_wait(barrier, expected)

    for step in steps:

        @pl.when(exists(step))
        def _():
            for copy in copies(step):
                copy.start()

    for step in steps:

        @pl.when(exists((-step[0], -step[1])))
        def _():
            for copy in copies(step):
                copy.wait_recv()

    for t in range(1, slabs + 3):
        inside = 2 <= t < slabs + 2
        first, count = (TILE - 1, rows + 2) if inside else (TILE, rows)
        inv_rho = 1.0 / state[0, t, pl.ds(first, count)]
        mid, rate = rates(state, t, first, count, inv_rho)
        for f in range(FIELDS):
            mid_state[f, t, pl.ds(first, count)] = mid[f] + TIME_STEP * rate[f]

    for at, edge in ((1, theta == 0), (slabs + 2, theta == n_theta - 1)):

        @pl.when(edge)
        def _():
            for f in range(FIELDS):
                mid_state[f, at, own_r] = jnp.zeros((rows, lanes), jnp.float32)

    for at, edge in ((TILE - 1, row == 0), (TILE + rows, row == n_row - 1)):

        @pl.when(edge)
        def _():
            for f in range(FIELDS):
                mid_state[f, own_t, pl.ds(at, 1)] = jnp.zeros((slabs, 1, lanes), jnp.float32)

    for t in range(slabs):
        inv_rho = 1.0 / state[0, t + 2, own_r]
        mid, rate = rates(mid_state, t + 2, TILE, rows, inv_rho)
        for f in range(FIELDS):
            ring[phi, t, f] = 0.5 * (state[f, t + 2, own_r] + mid[f] + TIME_STEP * rate[f])

    half = slabs // 2
    parts = [pl.ds(0, half), pl.ds(half, slabs - half)]

    def hop(way, distance, part):
        sign = 1 if way == 0 else -1
        slot = lax.rem(phi + n_phi - sign * (distance - 1), n_phi)
        return pltpu.make_async_remote_copy(
            src_ref=ring.at[slot, parts[part]],
            dst_ref=ring.at[slot, parts[part]],
            send_sem=ring_send.at[way, distance - 1, part],
            recv_sem=ring_recv.at[way, distance - 1, part],
            device_id={"phi": ahead_phi if way == 0 else back_phi},
            device_id_type=MESH,
        )

    last = n_phi // 2
    sends = []
    for distance in range(1, last + 1):
        for order in (0, 1):
            for way in (0, 1):
                part = order ^ way
                if distance > 1:
                    hop(way, distance - 1, part).wait_recv()
                if distance == last and n_phi % 2 == 0 and order == 1:
                    continue
                sends.append(hop(way, distance, part))
                sends[-1].start()
    if n_phi > 1:
        for order in (0, 1):
            for way in (0, 1):
                if n_phi % 2 == 0 and order == 1:
                    continue
                hop(way, last, order ^ way).wait_recv()

    lane = lax.broadcasted_iota(jnp.int32, (rows, lanes), 1)
    line = lax.broadcasted_iota(jnp.int32, (rows, lanes), 0)
    hops = jnp.zeros((rows, lanes), jnp.int32)
    rest = jnp.zeros((rows, lanes), jnp.int32)
    visc = jnp.zeros((rows, lanes), jnp.float32)
    for r in range(rows):
        shift = shifts[r]
        count = lax.div(shift, lanes)
        hops = jnp.where(line == r, count, hops)
        rest = jnp.where(line == r, shift - count * lanes, rest)
        visc = jnp.where(line == r, viscosity[r], visc)
    near = phi - hops
    near = jnp.where(near < 0, near + n_phi, near)
    far = jnp.where(near == 0, n_phi - 1, near - 1)
    next_ = jnp.where(near == n_phi - 1, 0, near + 1)
    from_near = lane < lanes - rest
    whole_first = (rest == 0) & (lane == 0)
    main_slot = jnp.where(from_near, near, far)
    side_slot = jnp.where(from_near, jnp.where(whole_first, next_, far), near)
    index = jnp.where(lane >= rest, lane - rest, lane - rest + lanes)

    def turned(slot_of, t, f):
        value = ring[0, t, f]
        for slot in range(1, n_phi):
            value = jnp.where(slot_of == slot, ring[slot, t, f], value)
        return jnp.take_along_axis(value, index, axis=1, mode="promise_in_bounds")

    for t in range(slabs):
        dens = turned(main_slot, t, 0)
        ener = turned(main_slot, t, 1)
        density_out[t] = dens
        for f in range(3):
            here = turned(main_slot, t, 2 + f)
            side = turned(side_slot, t, 2 + f)
            behind = pltpu.roll(jnp.where(lane == lanes - 1, side, here), 1, 1)
            ahead = pltpu.roll(jnp.where(lane == 0, side, here), lanes - 1, 1)
            velocity_out[f, t] = here + visc * (ahead - 2.0 * here + behind)
            if f == 2:
                slope = 0.5 * (ahead - behind)
                energy_out[t] = ener + visc * dens * slope * slope

    for step in steps:

        @pl.when(exists(step))
        def _():
            for copy in copies(step):
                copy.wait_send()

    for send in sends:
        send.wait_send()


def per_device(sizes, density, energy, velocity, shifts, viscosity):
    slabs, rows, lanes = density.shape
    n_phi = sizes[0]
    padded = (FIELDS, slabs + 4, rows + 2 * TILE, lanes)
    in_vmem = pl.BlockSpec(memory_space=pltpu.VMEM)
    in_smem = pl.BlockSpec(memory_space=pltpu.SMEM)
    reach = max(n_phi // 2, 1)
    return pl.pallas_call(
        functools.partial(kernel, sizes),
        out_shape=[jax.ShapeDtypeStruct(v.shape, v.dtype) for v in (density, energy, velocity)],
        in_specs=[in_smem, in_smem, in_vmem, in_vmem, in_vmem],
        out_specs=[in_vmem] * 3,
        scratch_shapes=[
            pltpu.VMEM(padded, jnp.float32),
            pltpu.VMEM(padded, jnp.float32),
            pltpu.VMEM((n_phi, slabs, FIELDS, rows, lanes), jnp.float32),
            pltpu.SemaphoreType.DMA((8, 3)),
            pltpu.SemaphoreType.DMA((8, 3)),
            pltpu.SemaphoreType.DMA((2, reach, 2)),
            pltpu.SemaphoreType.DMA((2, reach, 2)),
        ],
        compiler_params=pltpu.CompilerParams(collective_id=0, has_side_effects=True),
        name="disc_step",
    )(shifts, viscosity, density, energy, velocity)


def solution(mesh):
    sizes = tuple(mesh.shape[a] for a in ("phi", "row", "theta"))
    cells = P("theta", "row", "phi")
    vectors = P(None, "theta", "row", "phi")
    return jax.shard_map(
        functools.partial(per_device, sizes),
        mesh=mesh,
        in_specs=(cells, cells, vectors, P("row"), P("row")),
        out_specs=(cells, cells, vectors),
        check_vma=False,
    )
```
